512 devices in a mesh: dp: 32 (over y, z_hi, core), tensor: 16 (over z_lo, x).
Axes of the slice: x: 4, y: 4, z: 16 (z_hi: 4, z_lo: 4; z = z_hi * 4 + z_lo), core: 2. Of those that a mesh axis runs over, the one named last changes fastest.
Arguments:
- acts: bfloat16 [12288, 4096], P('dp', 'tensor'), may hold values from -6 to 6
- grad_out: bfloat16 [12288, 4096], P('dp', 'tensor'), may hold values from -60 to 60
- gate_pre: bfloat16 [12288, 14336], P('dp', 'tensor'), may hold values from -6 to 6
- up_pre: bfloat16 [12288, 14336], P('dp', 'tensor'), may hold values from -6 to 6
- down_weight: bfloat16 [14336, 4096], P('tensor', 'dp'), may hold values from -0.09375 to 0.09375
- proj_in: bfloat16 [4096, 64], P('tensor'), may hold values from -0.09375 to 0.09375
- proj_out: bfloat16 [14336, 64], P('tensor'), may hold values from -0.046875 to 0.046875
- lengths: int32 [96], P('dp'), may hold values from 64 to 128
- query_ids: int32 [16], replicated, may hold values from 0 to 95
Outputs:
- gram: float32 [4096, 4096], P('dp', 'tensor')
- scores: float32 [16, 96], P(None, 'dp')
The draws below stay inside these ranges and needn't reach their ends.
Inputs may be any that keep to these rules, and one draw needn't show every extreme that they name: `query_ids`: queries may repeat.
All inputs are finite; a program needn't handle non-finite values.
Results may differ from the reference program's by a relative error of at most 0.004.
Values may be sent and summed in bfloat16 or wider, within the bound.
No kernel may reach another device: no remote copies, remote signals or barrier semaphores. Data moves between devices by JAX's collectives and lax.ppermute only.
A program may use at most 64 MiB of HBM per device.

```python
import jax
import jax.numpy as jnp
from jax import lax

D = 4096
FF = 14336
KI = 64
KO = 64
SEQ = 128
Q = 16
EXAMPLES = 96
TOKENS = 12288
FEAT = 4096


def draw_grad_out(key, part):
    key = jax.random.fold_in(key, 101)
    total_rows = EXAMPLES * SEQ
    example = jnp.arange(total_rows) // SEQ
    ramp = example.astype(jnp.float32) / EXAMPLES
    values = jnp.clip(jax.random.normal(key, (total_rows, D), jnp.float32), -6.0, 6.0)
    factor = jnp.power(10.0, ramp)
    return (values * factor[:, None]).astype(jnp.bfloat16)


def draw_acts(key, part):
    key = jax.random.fold_in(key, 202)
    total_rows = EXAMPLES * SEQ
    values = jnp.clip(jax.random.normal(key, (total_rows, D), jnp.float32), -6.0, 6.0)
    return values.astype(jnp.bfloat16)


def draw_up_pre(key, part):
    key = jax.random.fold_in(key, 303)
    total_rows = EXAMPLES * SEQ
    values = jnp.clip(jax.random.normal(key, (total_rows, FF), jnp.float32), -6.0, 6.0)
    return values.astype(jnp.bfloat16)


def with_ends(entries, key, least, largest):
    index_at = [jax.random.randint(jax.random.fold_in(key, axis), (), 0, length) for axis, length in enumerate(entries.shape)]
    widest = entries.shape.index(max(entries.shape))
    neighbour = index_at[:widest] + [(index_at[widest] + 1) % entries.shape[widest]] + index_at[widest + 1:]
    return entries.at[tuple(index_at)].set(least).at[tuple(neighbour)].set(largest)


def level_of(own_key, shape, cuts, low, high):
    gain, own = 1.0, jax.random.fold_in(own_key, 6)
    for position, shards_of in cuts:
        steps = jnp.exp(jax.random.uniform(jax.random.fold_in(own, position), (shards_of,), jnp.float32, low / len(cuts), high / len(cuts)))
        gain = gain * jnp.repeat(steps, shape[position] // shards_of).reshape([-1 if axis == position else 1 for axis in range(len(shape))])
    return gain


def centred(stream_key, shape, width, bound, cuts=(), held_as=jnp.bfloat16):
    values = jax.random.normal(stream_key, shape, jnp.float32) * width
    if len(cuts) > 0:
        values = level_of(stream_key, shape, cuts, -0.22, 0.18) * values
    return jnp.clip(values, min=-bound, max=bound).astype(held_as)


def setup_inputs(seed: int = 0) -> dict:
    streams_of = jax.random.split(jax.random.key(seed), 10)
    acts = draw_acts(jax.random.fold_in(streams_of[9], 71), 0)
    grad_out = draw_grad_out(jax.random.fold_in(streams_of[9], 71), 0)
    gate_pre = centred(streams_of[2], (TOKENS, FF), 1.0, 6.0, ((0, 32), (1, 16)))
    up_pre = draw_up_pre(jax.random.fold_in(streams_of[9], 71), 0)
    down_weight = centred(streams_of[4], (FF, D), D ** -0.5, 0.09375, ((0, 16), (1, 32)))
    proj_in = centred(streams_of[5], (D, KI), D ** -0.5, 0.09375, ((0, 16),))
    proj_out = centred(streams_of[6], (FF, KO), FF ** -0.5, 0.046875, ((0, 16),))
    lengths = with_ends(jax.random.randint(streams_of[7], (EXAMPLES,), SEQ // 2, SEQ + 1), jax.random.fold_in(streams_of[7], 1), SEQ // 2, SEQ).astype(jnp.int32)
    query_ids = with_ends(jax.random.randint(streams_of[8], (Q,), 0, EXAMPLES), jax.random.fold_in(streams_of[8], 1), 0, EXAMPLES - 1).astype(jnp.int32)
    return {"acts": acts, "grad_out": grad_out, "gate_pre": gate_pre, "up_pre": up_pre, "down_weight": down_weight, "proj_in": proj_in, "proj_out": proj_out, "lengths": lengths, "query_ids": query_ids}


def silu_slope(value):
    sigma = jax.nn.sigmoid(value)
    return sigma + value * sigma * (1.0 - sigma)


def reference(acts, grad_out, gate_pre, up_pre, down_weight, proj_in, proj_out, lengths, query_ids):
    highest = lax.Precision.HIGHEST
    weight_full = down_weight.astype(jnp.float32)

    def one_example(items):
        act_rows, grad_rows, gate_rows, up_rows, length = items
        hidden_grad = jnp.dot(grad_rows.astype(jnp.float32), weight_full.T, precision=highest)
        gate_value = gate_rows.astype(jnp.float32)
        gate_grad = (hidden_grad * up_rows.astype(jnp.float32) * silu_slope(gate_value)).astype(jnp.bfloat16)
        out_factor = jnp.dot(gate_grad, proj_out, preferred_element_type=jnp.float32)
        in_factor = jnp.dot(act_rows, proj_in, preferred_element_type=jnp.float32)
        live = (jnp.arange(SEQ, dtype=jnp.int32) < length).astype(jnp.float32)
        out_factor = out_factor * live[:, None]
        return jnp.dot(out_factor.T, in_factor, precision=highest).reshape(-1)

    features = lax.map(one_example, (acts.reshape(EXAMPLES, SEQ, D), grad_out.reshape(EXAMPLES, SEQ, D),
                                     gate_pre.reshape(EXAMPLES, SEQ, FF), up_pre.reshape(EXAMPLES, SEQ, FF), lengths))
    norm_mean = jnp.sum(features * features) / EXAMPLES + 1e-6
    gram = jnp.dot(features.T, features, precision=highest) * (FEAT / EXAMPLES) / norm_mean
    query_feat = features[query_ids]
    scores = jnp.dot(query_feat, features.T, precision=highest) / norm_mean
    return gram, scores
```

```python
import functools

import jax
import jax.numpy as jnp
from jax import lax
from jax.experimental import pallas as pl
from jax.experimental.pallas import tpu as pltpu
from jax.sharding import Mesh
from jax.sharding import PartitionSpec as P


DP = ("y", "zh", "c")
TENSOR = ("zl", "x")
F32 = jnp.float32
BF16 = jnp.bfloat16
HIGH = lax.Precision.HIGHEST
NT = (((1,), (1,)), ((), ()))
VM = pl.BlockSpec(memory_space=pltpu.VMEM)
SM = pl.BlockSpec(memory_space=pltpu.SMEM)
ANY = pl.BlockSpec(memory_space=pl.ANY)


def shift(value, axis, by):
    count = lax.axis_size(axis)
    return lax.ppermute(value, axis, [(k, (k + by) % count) for k in range(count)])


def exchange(value, axis):
    return lax.all_to_all(value, axis, 0, 0, tiled=True)


def pack_rows(msg_ref, table, examples, per):
    seq = table.shape[1] // examples
    for j in range(msg_ref.shape[0]):
        for e in range(examples):
            msg_ref[j, e * per : (e + 1) * per, :] = table[
                j * per : (j + 1) * per, e * seq : (e + 1) * seq
            ]
        if msg_ref.shape[1] > examples * per:
            rest = msg_ref.shape[1] - examples * per
            msg_ref[j, examples * per :, :] = jnp.zeros((rest, seq), F32)


def in_kernel(examples, per, proj_ref, acts_ref, msg_ref):
    table = lax.dot_general(proj_ref[...], acts_ref[...], NT, preferred_element_type=F32)
    pack_rows(msg_ref, table, examples, per)


def slope_kernel(gate_ref, up_ref, out_ref):
    value = gate_ref[...].astype(F32)
    sigma = jax.nn.sigmoid(value)
    out_ref[...] = up_ref[...].astype(F32) * (sigma + value * sigma * (1.0 - sigma))


def times(ws, gs, g):
    left = jnp.concatenate([gs[g, z] for z in range(4)], axis=1)
    right = jnp.concatenate([ws[g, c, z] for z in range(4) for c in range(2)], axis=1)
    return lax.dot_general(left, right, NT, preferred_element_type=F32)


def most_kernel(where, w0, w1, w2, v0, v1, v2, g0, g1, g2, g3, acc_ref, ws, gs, sems):
    y, c = where[0], where[2]
    copies = []
    for g, (mine, other, step) in enumerate(((w0, v0, 0), (w1, v1, 3), (w2, v2, 1))):
        copies.append(
            [
                pltpu.make_async_copy(mine, ws.at[g, c], sems.at[g, 0]),
                pltpu.make_async_copy(other, ws.at[g, 1 - c], sems.at[g, 1]),
            ]
            + [
                pltpu.make_async_copy(
                    ref.at[lax.rem(y + step, 4)], gs.at[g, lax.rem(where[4] + k, 4)], sems.at[g, 2 + k]
                )
                for k, ref in enumerate((g0, g1, g2, g3))
            ]
        )
    for group in copies:
        for copy in group:
            copy.start()
    for g, group in enumerate(copies):
        for copy in group:
            copy.wait()
        part = times(ws, gs, g)
        acc_ref[...] = part if g == 0 else acc_ref[...] + part


def last_kernel(
    examples, per, where, q0, q1, r0, r1, g0, g1, g2, g3, acc_ref, slope_ref, proj_ref, msg_ref, ws, gs, sems
):
    y, c = where[0], where[2]
    copies = [
        pltpu.make_async_copy(q0, ws.at[0, c, pl.ds(0, 2)], sems.at[0]),
        pltpu.make_async_copy(q1, ws.at[0, c, pl.ds(2, 2)], sems.at[1]),
        pltpu.make_async_copy(r0, ws.at[0, 1 - c, pl.ds(0, 2)], sems.at[2]),
        pltpu.make_async_copy(r1, ws.at[0, 1 - c, pl.ds(2, 2)], sems.at[3]),
    ] + [
        pltpu.make_async_copy(
            ref.at[lax.rem(y + 2, 4)], gs.at[0, lax.rem(where[4] + k, 4)], sems.at[4 + k]
        )
        for k, ref in enumerate((g0, g1, g2, g3))
    ]
    for copy in copies:
        copy.start()
    for copy in copies:
        copy.wait()
    hidden = acc_ref[...] + times(ws, gs, 0)
    gate_grad = (hidden * slope_ref[...]).astype(BF16)
    table = lax.dot_general(proj_ref[...], gate_grad, NT, preferred_element_type=F32)
    pack_rows(msg_ref, table, examples, per)


def feature_kernel(examples, per, lengths, out_ref, in_ref, msg_ref):
    rows = jnp.sum(out_ref[...], axis=0)
    seq = rows.shape[1]
    position = lax.broadcasted_iota(jnp.int32, (per, seq), 1)
    lines = []
    for e in range(examples):
        left = jnp.where(position < lengths[e], rows[e * per : (e + 1) * per], 0.0)
        right = jnp.concatenate(
            [in_ref[j, e * per : (e + 1) * per, :] for j in range(in_ref.shape[0])], axis=0
        )
        part = lax.dot_general(left, right, NT, precision=HIGH, preferred_element_type=F32)
        for h in range(per // 2):
            lines.append(jnp.concatenate([part[2 * h : 2 * h + 1], part[2 * h + 1 : 2 * h + 2]], axis=1))
    lines.append(jnp.zeros((msg_ref.shape[1] - len(lines), 2 * part.shape[1]), F32))
    tile = jnp.concatenate(lines, axis=0)
    msg_ref[...] = jnp.broadcast_to(tile[None], msg_ref.shape)


def columns_of(all_ref, examples):
    return jnp.concatenate(
        [
            jnp.concatenate([all_ref[:, 2 * e, :], all_ref[:, 2 * e + 1, :]], axis=1)
            for e in range(examples)
        ],
        axis=0,
    )


def share_kernel(examples, where, pick_ref, all_ref, col_ref, msg_ref):
    cols = columns_of(all_ref, examples)
    col_ref[...] = cols
    count = cols.shape[0]
    half = cols.shape[1] // 2
    own = all_ref[where[5]]
    chosen = (
        pick_ref[...] == lax.broadcasted_iota(jnp.int32, (pick_ref.shape[0], count), 1)
    ).astype(F32)
    asked = jnp.dot(chosen, cols, precision=HIGH, preferred_element_type=F32)
    score = jnp.zeros((asked.shape[0], 128), F32)
    lane = lax.broadcasted_iota(jnp.int32, score.shape, 1)
    for e in range(examples):
        row = jnp.concatenate([own[2 * e : 2 * e + 1], own[2 * e + 1 : 2 * e + 2]], axis=1)
        value = jnp.sum(asked * row, axis=1, keepdims=True)
        score = jnp.where(lane == e, value, score)
    square = jnp.sum(jnp.sum(cols * cols, axis=1, keepdims=True), axis=0, keepdims=True)
    score = jnp.where(lane == examples, square, score)
    high = score.astype(BF16).astype(F32)
    low = score - high
    both = jnp.where(lane < 64, high, pltpu.roll(low, 64, 1)).astype(BF16)
    rows = jnp.where(lax.rem(where[5], 2) == 0, cols[:, :half], cols[:, half:]).astype(BF16)
    tile = jnp.concatenate([rows, both], axis=0)
    for j in range(msg_ref.shape[0]):
        msg_ref[j] = tile


def gram_kernel(examples, where, all_ref, col_ref, gram_ref, score_ref):
    cols = col_ref[...]
    count, width = cols.shape
    rows = all_ref[lax.div(where[5], 2), :count, :].astype(F32)
    both = jnp.sum(all_ref[:, count:, :].astype(F32), axis=0)
    score = both + pltpu.roll(both, 64, 1)
    total = score[0:1, examples : examples + 1]
    norm = total / count + 1e-06
    block = lax.dot_general(
        rows, cols, (((0,), (0,)), ((), ())), precision=HIGH, preferred_element_type=F32
    )
    gram_ref[...] = block * (width * all_ref.shape[0] / count) / norm
    score_ref[...] = (score / norm)[:, :examples]


def step(acts, grad_out, gate_pre, up_pre, down_weight, proj_in, proj_out, lengths, query_ids):
    tokens, ff_here = gate_pre.shape
    examples = lengths.shape[0]
    tensor = lax.axis_size(TENSOR)
    groups = lax.axis_size(DP)
    ko = proj_out.shape[1]
    per = ko // tensor
    index = [lax.axis_index(a) for a in ("y", "zh", "c", "zl", "x")]
    where = jnp.stack(index + [lax.axis_index(DP)]).astype(jnp.int32)
    msg = jax.ShapeDtypeStruct((tensor, 16, 128), F32)

    gz = lax.all_gather(grad_out, "zl")
    gz, down_weight = lax.optimization_barrier((gz, down_weight))
    wz = lax.all_gather(down_weight, "zh")
    gx = [gz]
    for k in (1, 2, 3):
        gx.append(shift(gz, "x", -k))
    wp = shift(wz, "y", 1)
    wm = shift(wz, "y", -1)
    q0 = shift(wp[:2], "y", 1)
    q1 = shift(wm[2:], "y", -1)
    cz, cp, cm = shift(wz, "c", 1), shift(wp, "c", 1), shift(wm, "c", 1)
    r0, r1 = shift(q0, "c", 1), shift(q1, "c", 1)

    in_msg = pl.pallas_call(
        functools.partial(in_kernel, examples, per), out_shape=msg, in_specs=[VM, VM], out_specs=VM
    )(proj_in.T, acts)
    in_own = jnp.sum(exchange(in_msg, TENSOR), axis=0)
    in_all = exchange(jnp.broadcast_to(in_own[None], (tensor, *in_own.shape)), TENSOR)
    slope = pl.pallas_call(
        slope_kernel,
        out_shape=jax.ShapeDtypeStruct((tokens, ff_here), F32),
        in_specs=[VM, VM],
        out_specs=VM,
    )(gate_pre, up_pre)
    gshape = (4, tokens, grad_out.shape[1])
    wshape = (2, 4, *down_weight.shape)
    acc = pl.pallas_call(
        most_kernel,
        out_shape=jax.ShapeDtypeStruct((tokens, ff_here), F32),
        in_specs=[SM] + [ANY] * 10,
        out_specs=VM,
        scratch_shapes=[
            pltpu.VMEM((3, *wshape), BF16),
            pltpu.VMEM((3, *gshape), BF16),
            pltpu.SemaphoreType.DMA((3, 6)),
        ],
    )(where, wz, wp, wm, cz, cp, cm, *gx)
    out_msg = pl.pallas_call(
        functools.partial(last_kernel, examples, per),
        out_shape=msg,
        in_specs=[SM] + [ANY] * 8 + [VM] * 3,
        out_specs=VM,
        scratch_shapes=[
            pltpu.VMEM((1, *wshape), BF16),
            pltpu.VMEM((1, *gshape), BF16),
            pltpu.SemaphoreType.DMA((8,)),
        ],
    )(where, q0, q1, r0, r1, *gx, acc, slope, proj_out.T)
    out_all = exchange(out_msg, TENSOR)
    piece = pl.pallas_call(
        functools.partial(feature_kernel, examples, per),
        out_shape=jax.ShapeDtypeStruct((groups, 8, 128), F32),
        in_specs=[SM, VM, VM],
        out_specs=VM,
    )(lengths, out_all, in_all)
    pieces = exchange(piece, DP)
    count = examples * groups
    pick = ((query_ids % examples) * groups + query_ids // examples)[:, None]
    queries = query_ids.shape[0]
    cols, row_msg = pl.pallas_call(
        functools.partial(share_kernel, examples),
        out_shape=(
            jax.ShapeDtypeStruct((count, 256), F32),
            jax.ShapeDtypeStruct((tensor, count + queries, 128), BF16),
        ),
        in_specs=[SM, VM, VM],
        out_specs=(VM, VM),
    )(where, pick, pieces)
    row_all = exchange(row_msg, TENSOR)
    gram, scores = pl.pallas_call(
        functools.partial(gram_kernel, examples),
        out_shape=(
            jax.ShapeDtypeStruct((128, 256), F32),
            jax.ShapeDtypeStruct((queries, examples), F32),
        ),
        in_specs=[SM, VM, VM],
        out_specs=(VM, VM),
    )(where, row_all, cols)
    return gram, scores


def solution(mesh):
    split = Mesh(mesh.devices.reshape(4, 4, 2, 4, 4), (*DP, *TENSOR))
    in_specs = (
        P(DP, TENSOR),
        P(DP, TENSOR),
        P(DP, TENSOR),
        P(DP, TENSOR),
        P(TENSOR, DP),
        P(TENSOR, None),
        P(TENSOR, None),
        P(DP),
        P(),
    )
    out_specs = (P(DP, TENSOR), P(None, DP))
    return jax.shard_map(step, mesh=split, in_specs=in_specs, out_specs=out_specs, check_vma=False)
```

```python
import functools

import jax
import jax.numpy as jnp
from jax import lax
from jax.experimental import pallas as pl
from jax.experimental.pallas import tpu as pltpu
from jax.sharding import Mesh
from jax.sharding import PartitionSpec as P


DP = ("y", "zh", "c")
TENSOR = ("zl", "x")
F32 = jnp.float32
BF16 = jnp.bfloat16
HIGH = lax.Precision.HIGHEST
NT = (((1,), (1,)), ((), ()))
SMALL = pltpu.CompilerParams(vmem_limit_bytes=8 << 20)
LARGE = pltpu.CompilerParams(vmem_limit_bytes=24 << 20)
VM = pl.BlockSpec(memory_space=pltpu.VMEM)
SM = pl.BlockSpec(memory_space=pltpu.SMEM)
ANY = pl.BlockSpec(memory_space=pl.ANY)


def shift(value, axis, by):
    count = lax.axis_size(axis)
    return lax.ppermute(value, axis, [(k, (k + by) % count) for k in range(count)])


def exchange(value, axis):
    return lax.all_to_all(value, axis, 0, 0, tiled=True)


def pack_rows(msg_ref, table, examples, per):
    seq = table.shape[1] // examples
    for j in range(msg_ref.shape[0]):
        for e in range(examples):
            msg_ref[j, e * per : (e + 1) * per, :] = table[
                j * per : (j + 1) * per, e * seq : (e + 1) * seq
            ]
        if msg_ref.shape[1] > examples * per:
            rest = msg_ref.shape[1] - examples * per
            msg_ref[j, examples * per :, :] = jnp.zeros((rest, seq), F32)


def in_kernel(examples, per, proj_ref, acts_ref, msg_ref):
    table = lax.dot_general(proj_ref[...], acts_ref[...], NT, preferred_element_type=F32)
    pack_rows(msg_ref, table, examples, per)


def slope_kernel(gate_ref, up_ref, out_ref):
    value = gate_ref[...].astype(F32)
    sigma = jax.nn.sigmoid(value)
    out_ref[...] = up_ref[...].astype(F32) * (sigma + value * sigma * (1.0 - sigma))


def times(ws, gs, g):
    left = jnp.concatenate([gs[g, z] for z in range(4)], axis=1)
    right = jnp.concatenate([ws[g, c, z] for z in range(4) for c in range(2)], axis=1)
    return lax.dot_general(left, right, NT, preferred_element_type=F32)


def most_kernel(where, w0, w1, w2, v0, v1, v2, g0, g1, g2, g3, acc_ref, ws, gs, sems):
    y, c = where[0], where[2]
    copies = []
    for g, (mine, other, step) in enumerate(((w0, v0, 0), (w1, v1, 3), (w2, v2, 1))):
        copies.append(
            [
                pltpu.make_async_copy(mine, ws.at[g, c], sems.at[g, 0]),
                pltpu.make_async_copy(other, ws.at[g, 1 - c], sems.at[g, 1]),
            ]
            + [
                pltpu.make_async_copy(
                    ref.at[lax.rem(y + step, 4)], gs.at[g, lax.rem(where[4] + k, 4)], sems.at[g, 2 + k]
                )
                for k, ref in enumerate((g0, g1, g2, g3))
            ]
        )
    for group in copies:
        for copy in group:
            copy.start()
    for g, group in enumerate(copies):
        for copy in group:
            copy.wait()
        part = times(ws, gs, g)
        acc_ref[...] = part if g == 0 else acc_ref[...] + part


def last_kernel(
    examples, per, where, q0, q1, r0, r1, g0, g1, g2, g3, acc_ref, slope_ref, proj_ref, msg_ref, ws, gs, sems
):
    y, c = where[0], where[2]
    copies = [
        pltpu.make_async_copy(q0, ws.at[0, c, pl.ds(0, 2)], sems.at[0]),
        pltpu.make_async_copy(q1, ws.at[0, c, pl.ds(2, 2)], sems.at[1]),
        pltpu.make_async_copy(r0, ws.at[0, 1 - c, pl.ds(0, 2)], sems.at[2]),
        pltpu.make_async_copy(r1, ws.at[0, 1 - c, pl.ds(2, 2)], sems.at[3]),
    ] + [
        pltpu.make_async_copy(
            ref.at[lax.rem(y + 2, 4)], gs.at[0, lax.rem(where[4] + k, 4)], sems.at[4 + k]
        )
        for k, ref in enumerate((g0, g1, g2, g3))
    ]
    for copy in copies:
        copy.start()
    for copy in copies:
        copy.wait()
    hidden = acc_ref[...] + times(ws, gs, 0)
    gate_grad = (hidden * slope_ref[...]).astype(BF16)
    table = lax.dot_general(proj_ref[...], gate_grad, NT, preferred_element_type=F32)
    pack_rows(msg_ref, table, examples, per)


def feature_kernel(examples, per, lengths, out_ref, in_ref, msg_ref):
    rows = jnp.sum(out_ref[...], axis=0)
    seq = rows.shape[1]
    position = lax.broadcasted_iota(jnp.int32, (per, seq), 1)
    lines = []
    for e in range(examples):
        left = jnp.where(position < lengths[e], rows[e * per : (e + 1) * per], 0.0)
        right = jnp.concatenate(
            [in_ref[j, e * per : (e + 1) * per, :] for j in range(in_ref.shape[0])], axis=0
        )
        part = lax.dot_general(left, right, NT, precision=HIGH, preferred_element_type=F32)
        for h in range(per // 2):
            lines.append(jnp.concatenate([part[2 * h : 2 * h + 1], part[2 * h + 1 : 2 * h + 2]], axis=1))
    lines.append(jnp.zeros((msg_ref.shape[1] - len(lines), 2 * part.shape[1]), F32))
    tile = jnp.concatenate(lines, axis=0)
    msg_ref[...] = jnp.broadcast_to(tile[None], msg_ref.shape)


def columns_of(all_ref, examples):
    return jnp.concatenate(
        [
            jnp.concatenate([all_ref[:, 2 * e, :], all_ref[:, 2 * e + 1, :]], axis=1)
            for e in range(examples)
        ],
        axis=0,
    )


def share_kernel(examples, where, pick_ref, all_ref, col_ref, msg_ref):
    cols = columns_of(all_ref, examples)
    col_ref[...] = cols
    count = cols.shape[0]
    half = cols.shape[1] // 2
    own = all_ref[where[5]]
    chosen = (
        pick_ref[...] == lax.broadcasted_iota(jnp.int32, (pick_ref.shape[0], count), 1)
    ).astype(F32)
    asked = jnp.dot(chosen, cols, precision=HIGH, preferred_element_type=F32)
    score = jnp.zeros((asked.shape[0], 128), F32)
    lane = lax.broadcasted_iota(jnp.int32, score.shape, 1)
    for e in range(examples):
        row = jnp.concatenate([own[2 * e : 2 * e + 1], own[2 * e + 1 : 2 * e + 2]], axis=1)
        value = jnp.sum(asked * row, axis=1, keepdims=True)
        score = jnp.where(lane == e, value, score)
    square = jnp.sum(jnp.sum(cols * cols, axis=1, keepdims=True), axis=0, keepdims=True)
    score = jnp.where(lane == examples, square, score)
    high = score.astype(BF16).astype(F32)
    low = score - high
    both = jnp.where(lane < 64, high, pltpu.roll(low, 64, 1)).astype(BF16)
    rows = jnp.where(lax.rem(where[5], 2) == 0, cols[:, :half], cols[:, half:]).astype(BF16)
    tile = jnp.concatenate([rows, both], axis=0)
    for j in range(msg_ref.shape[0]):
        msg_ref[j] = tile


def gram_kernel(examples, where, all_ref, col_ref, gram_ref, score_ref):
    cols = col_ref[...]
    count, width = cols.shape
    rows = all_ref[lax.div(where[5], 2), :count, :].astype(F32)
    both = jnp.sum(all_ref[:, count:, :].astype(F32), axis=0)
    score = both + pltpu.roll(both, 64, 1)
    total = score[0:1, examples : examples + 1]
    norm = total / count + 1e-06
    block = lax.dot_general(
        rows, cols, (((0,), (0,)), ((), ())), precision=HIGH, preferred_element_type=F32
    )
    gram_ref[...] = block * (width * all_ref.shape[0] / count) / norm
    score_ref[...] = (score / norm).T[:examples]


def step(acts, grad_out, gate_pre, up_pre, down_weight, proj_in, proj_out, lengths, query_ids):
    tokens, ff_here = gate_pre.shape
    examples = lengths.shape[0]
    tensor = lax.axis_size(TENSOR)
    groups = lax.axis_size(DP)
    ko = proj_out.shape[1]
    per = ko // tensor
    index = [lax.axis_index(a) for a in ("y", "zh", "c", "zl", "x")]
    where = jnp.stack(index + [lax.axis_index(DP)]).astype(jnp.int32)
    msg = jax.ShapeDtypeStruct((tensor, 16, 128), F32)

    gz = lax.all_gather(grad_out, "zl")
    gz, down_weight = lax.optimization_barrier((gz, down_weight))
    wz = lax.all_gather(down_weight, "zh")
    gx = [gz]
    for k in (1, 2, 3):
        gx.append(shift(gz, "x", -k))
    wp = shift(wz, "y", 1)
    wm = shift(wz, "y", -1)
    q0 = shift(wp[:2], "y", 1)
    q1 = shift(wm[2:], "y", -1)
    cz = shift(wz, "c", 1)
    cp = shift(wp, "c", 1)
    cm = shift(wm, "c", 1)
    r0, r1 = shift(q0, "c", 1), shift(q1, "c", 1)

    in_msg = pl.pallas_call(
        functools.partial(in_kernel, examples, per), out_shape=msg, in_specs=[VM, VM], out_specs=VM, compiler_params=SMALL
    )(proj_in.T, acts)
    in_own = jnp.sum(exchange(in_msg, TENSOR), axis=0)
    in_all = exchange(jnp.broadcast_to(in_own[None], (tensor, *in_own.shape)), TENSOR)
    slope = pl.pallas_call(
        slope_kernel,
        out_shape=jax.ShapeDtypeStruct((tokens, ff_here), F32),
        compiler_params=SMALL,
        in_specs=[VM, VM],
        out_specs=VM,
    )(gate_pre, up_pre)
    gshape = (4, tokens, grad_out.shape[1])
    wshape = (2, 4, *down_weight.shape)
    acc = pl.pallas_call(
        most_kernel,
        out_shape=jax.ShapeDtypeStruct((tokens, ff_here), F32),
        compiler_params=LARGE,
        in_specs=[SM] + [ANY] * 10,
        out_specs=VM,
        scratch_shapes=[
            pltpu.VMEM((3, *wshape), BF16),
            pltpu.VMEM((3, *gshape), BF16),
            pltpu.SemaphoreType.DMA((3, 6)),
        ],
    )(where, wz, wp, wm, cz, cp, cm, *gx)
    out_msg = pl.pallas_call(
        functools.partial(last_kernel, examples, per),
        out_shape=msg,
        compiler_params=LARGE,
        in_specs=[SM] + [ANY] * 8 + [VM] * 3,
        out_specs=VM,
        scratch_shapes=[
            pltpu.VMEM((1, *wshape), BF16),
            pltpu.VMEM((1, *gshape), BF16),
            pltpu.SemaphoreType.DMA((8,)),
        ],
    )(where, q0, q1, r0, r1, *gx, acc, slope, proj_out.T)
    out_all = exchange(out_msg, TENSOR)
    piece = pl.pallas_call(
        functools.partial(feature_kernel, examples, per),
        out_shape=jax.ShapeDtypeStruct((groups, 8, 128), F32),
        compiler_params=SMALL,
        in_specs=[SM, VM, VM],
        out_specs=VM,
    )(lengths, out_all, in_all)
    pieces = exchange(piece, DP)
    count = examples * groups
    pick = ((query_ids % examples) * groups + query_ids // examples)[:, None]
    queries = query_ids.shape[0]
    cols, row_msg = pl.pallas_call(
        functools.partial(share_kernel, examples),
        out_shape=(
            jax.ShapeDtypeStruct((count, 256), F32),
            jax.ShapeDtypeStruct((tensor, count + queries, 128), BF16),
        ),
        compiler_params=SMALL,
        in_specs=[SM, VM, VM],
        out_specs=(VM, VM),
    )(where, pick, pieces)
    row_all = exchange(row_msg, TENSOR)
    gram, scores = pl.pallas_call(
        functools.partial(gram_kernel, examples),
        out_shape=(
            jax.ShapeDtypeStruct((128, 256), F32),
            jax.ShapeDtypeStruct((examples, queries), F32),
        ),
        compiler_params=SMALL,
        in_specs=[SM, VM, VM],
        out_specs=(VM, VM),
    )(where, row_all, cols)
    return gram, scores.T


def solution(mesh):
    split = Mesh(mesh.devices.reshape(4, 4, 2, 4, 4), (*DP, *TENSOR))
    in_specs = (
        P(DP, TENSOR),
        P(DP, TENSOR),
        P(DP, TENSOR),
        P(DP, TENSOR),
        P(TENSOR, DP),
        P(TENSOR, None),
        P(TENSOR, None),
        P(DP),
        P(),
    )
    out_specs = (P(DP, TENSOR), P(None, DP))
    return jax.shard_map(step, mesh=split, in_specs=in_specs, out_specs=out_specs, check_vma=False)
```
